256 devices in a mesh: row: 8 (over x, y_hi), col: 32 (over z, y_lo, core).
Axes of the slice: x: 4, y: 4 (y_hi: 2, y_lo: 2; y = y_hi * 2 + y_lo), z: 8, core: 2. Of those that a mesh axis runs over, the one named last changes fastest.
Arguments:
- e_field: float32 [3, 64, 64, 4096], P(None, None, 'row', 'col'), may hold values from -6 to 6
- h_field: float32 [3, 64, 64, 4096], P(None, None, 'row', 'col'), may hold values from -6 to 6
- e_coef: float32 [64, 64, 4096], P(None, 'row', 'col'), may hold values from 0.125 to 0.5
- basis: float32 [128, 64, 4096], P('row', None, 'col'), may hold values from -0.01171875 to 0.01171875
- pml_width: int32 [4], replicated, may hold values from 2 to 8
- snap_index: int32 [64], replicated, may hold values from 0 to 383
Outputs:
- e_final: float32 [3, 64, 64, 4096], P(None, None, 'row', 'col')
- h_final: float32 [3, 64, 64, 4096], P(None, None, 'row', 'col')
- coefficients: float32 [64, 128], replicated
- gram: float32 [64, 64], replicated
The draws below stay inside these ranges and needn't reach their ends.
All inputs are finite; a program needn't handle non-finite values.
Results may differ from the reference program's by a relative error of at most 0.00008.
Values sent between devices are 32-bit elements; how exact they have to be, the bound alone decides.
No kernel may reach another device: no remote copies, remote signals or barrier semaphores. Data moves between devices by JAX's collectives and lax.ppermute only.
A program may use at most 64 MiB of HBM per device.

```python
import math
import jax
import jax.numpy as jnp
from jax import lax

NZ = 64
STEPS = 8
RANK = 128
SNAPS = 64
NX = 64
NY = 4096


def place_ends(entries, own_key, low, high):
    spot = [jax.random.randint(jax.random.fold_in(own_key, axis), (), 0, length) for axis, length in enumerate(entries.shape)]
    main_axis = entries.shape.index(max(entries.shape))
    next_to = spot[:main_axis] + [(spot[main_axis] + 1) % entries.shape[main_axis]] + spot[main_axis + 1:]
    return entries.at[tuple(spot)].set(low).at[tuple(next_to)].set(high)


def level_of(rng, shape, shards, smallest, top_value):
    level, own = 1.0, jax.random.fold_in(rng, 6)
    for position, blocks in shards:
        draws = jnp.exp(jax.random.uniform(jax.random.fold_in(own, position), (blocks,), jnp.float32, smallest / len(shards), top_value / len(shards)))
        level = level * jnp.repeat(draws, shape[position] // blocks).reshape([-1 if axis == position else 1 for axis in range(len(shape))])
    return level


def normal_values(own_key, dims, width, limit, cuts=(), held_as=jnp.bfloat16):
    result = jax.random.normal(own_key, dims, jnp.float32) * width
    if len(cuts) > 0:
        result = level_of(own_key, dims, cuts, -0.22, 0.18) * result
    return jnp.clip(result, min=-limit, max=limit).astype(held_as)


def setup_inputs(seed: int = 0) -> dict:
    key_list = jax.random.split(jax.random.key(seed), 7)
    e_field = normal_values(key_list[0], (3, NZ, NX, NY), 1.0, 6.0, ((2, 8), (3, 32)), jnp.float32)
    h_field = normal_values(key_list[1], (3, NZ, NX, NY), 1.0, 6.0, ((2, 8), (3, 32)), jnp.float32)
    e_coef = jnp.clip(jnp.exp(math.log(0.5) - 1.3862944 * jax.random.uniform(key_list[2], (NZ, NX, NY), jnp.float32) ** level_of(key_list[2], (NZ, NX, NY), ((1, 8), (2, 32)), -0.2, 0.2)), 0.125, 0.5)
    basis = normal_values(key_list[3], (RANK, NX, NY), (NX * NY) ** -0.5, 0.01171875, ((0, 8), (2, 32)), jnp.float32)
    pml_width = place_ends(jax.random.randint(key_list[4], (4,), 2, 9), jax.random.fold_in(key_list[4], 1), 2, 8).astype(jnp.int32)
    snap_index = place_ends(jax.random.randint(key_list[5], (SNAPS,), 0, 6 * NZ), jax.random.fold_in(key_list[5], 1), 0, (6 * NZ) - 1).astype(jnp.int32)
    return {"e_field": e_field, "h_field": h_field, "e_coef": e_coef, "basis": basis, "pml_width": pml_width, "snap_index": snap_index}


time_step = 0.5
sigma_top = 4.0
alpha_shift = 0.05


def forward(field, axis, plane):
    count = field.shape[axis]
    after = jnp.concatenate([lax.slice_in_dim(field, 1, count, axis=axis), jnp.expand_dims(plane, axis)], axis)
    return after - field


def backward(field, axis, plane):
    count = field.shape[axis]
    before = jnp.concatenate([jnp.expand_dims(plane, axis), lax.slice_in_dim(field, 0, count - 1, axis=axis)], axis)
    return field - before


def absorber(positions, total, low, high):
    depth = jnp.maximum(jnp.maximum((low - positions) / low, (positions - (total - 1.0 - high)) / high), 0.0)
    sigma = sigma_top * depth ** 3
    damp = jnp.exp(-(sigma + alpha_shift) * time_step)
    gain = sigma / (sigma + alpha_shift) * (damp - 1.0)
    return damp, gain


def magnetic(e_field, h_field, psi, next_x, next_y, damp_x, gain_x, damp_y, gain_y):
    e_x, e_y, e_z = e_field[0], e_field[1], e_field[2]
    h_x, h_y, h_z = h_field[0], h_field[1], h_field[2]
    zplane = jnp.zeros_like(e_x[0])
    ez_dy = forward(e_z, 2, next_y[1])
    ey_dz = forward(e_y, 0, zplane)
    ex_dz = forward(e_x, 0, zplane)
    ez_dx = forward(e_z, 1, next_x[1])
    ey_dx = forward(e_y, 1, next_x[0])
    ex_dy = forward(e_x, 2, next_y[0])
    psi_hxy = damp_y * psi[0] + gain_y * ez_dy
    psi_hyx = damp_x * psi[1] + gain_x * ez_dx
    psi_hzx = damp_x * psi[2] + gain_x * ey_dx
    psi_hzy = damp_y * psi[3] + gain_y * ex_dy
    h_x = h_x - time_step * (ez_dy + psi_hxy - ey_dz)
    h_y = h_y - time_step * (ex_dz - ez_dx - psi_hyx)
    h_z = h_z - time_step * (ey_dx + psi_hzx - ex_dy - psi_hzy)
    return jnp.stack((h_x, h_y, h_z)), (psi_hxy, psi_hyx, psi_hzx, psi_hzy)


def electric(e_field, h_field, psi, e_coef, prev_x, prev_y, damp_x, gain_x, damp_y, gain_y):
    e_x, e_y, e_z = e_field[0], e_field[1], e_field[2]
    h_x, h_y, h_z = h_field[0], h_field[1], h_field[2]
    zplane = jnp.zeros_like(h_x[0])
    hz_dy = backward(h_z, 2, prev_y[1])
    hy_dz = backward(h_y, 0, zplane)
    hx_dz = backward(h_x, 0, zplane)
    hz_dx = backward(h_z, 1, prev_x[1])
    hy_dx = backward(h_y, 1, prev_x[0])
    hx_dy = backward(h_x, 2, prev_y[0])
    psi_exy = damp_y * psi[0] + gain_y * hz_dy
    psi_eyx = damp_x * psi[1] + gain_x * hz_dx
    psi_ezx = damp_x * psi[2] + gain_x * hy_dx
    psi_ezy = damp_y * psi[3] + gain_y * hx_dy
    e_x = e_x + e_coef * (hz_dy + psi_exy - hy_dz)
    e_y = e_y + e_coef * (hx_dz - hz_dx - psi_eyx)
    e_z = e_z + e_coef * (hy_dx + psi_ezx - hx_dy - psi_ezy)
    return jnp.stack((e_x, e_y, e_z)), (psi_exy, psi_eyx, psi_ezx, psi_ezy)


def reference(e_field, h_field, e_coef, basis, pml_width, snap_index):
    widths = pml_width.astype(jnp.float32)
    x_pos = jnp.arange(NX, dtype=jnp.float32)
    y_pos = jnp.arange(NY, dtype=jnp.float32)
    hdx, hgx = absorber(x_pos + 0.5, float(NX), widths[0], widths[1])
    hdy, hgy = absorber(y_pos + 0.5, float(NY), widths[2], widths[3])
    edx, egx = absorber(x_pos, float(NX), widths[0], widths[1])
    edy, egy = absorber(y_pos, float(NY), widths[2], widths[3])
    hdx, hgx, edx, egx = [v.reshape(1, NX, 1) for v in (hdx, hgx, edx, egx)]
    hdy, hgy, edy, egy = [v.reshape(1, 1, NY) for v in (hdy, hgy, edy, egy)]
    zeros_cells = jnp.zeros((NZ, NX, NY), jnp.float32)
    psi_mag = (zeros_cells,) * 4
    psi_ele = (zeros_cells,) * 4
    plane_x = jnp.zeros((2, NZ, NY), jnp.float32)
    plane_y = jnp.zeros((2, NZ, NX), jnp.float32)
    for step in range(STEPS):
        h_field, psi_mag = magnetic(e_field, h_field, psi_mag, plane_x, plane_y, hdx, hgx, hdy, hgy)
        e_field, psi_ele = electric(e_field, h_field, psi_ele, e_coef, plane_x, plane_y, edx, egx, edy, egy)
    planes = jnp.concatenate((e_field, h_field), 0).reshape(6 * NZ, NX, NY)
    snaps = jnp.take(planes, snap_index, axis=0).reshape(SNAPS, NX * NY)
    coefficients = jnp.dot(snaps, basis.reshape(RANK, NX * NY).T, precision=lax.Precision.HIGHEST)
    gram = jnp.dot(snaps, snaps.T, precision=lax.Precision.HIGHEST) / float(NX * NY)
    return e_field, h_field, coefficients, gram
```

```python
import functools

import jax
import jax.numpy as jnp
from jax import lax
from jax.experimental import pallas as pl
from jax.experimental.pallas import tpu as pltpu
from jax.sharding import Mesh
from jax.sharding import PartitionSpec as P

STEPS = 8
ROW = ("row_0", "row_1")
COL = ("col_0", "col_1", "col_2")
NEAR = ("row_1", "col_1", "col_2")
FAR = ("row_0", "col_0")

time_step = 0.5
sigma_top = 4.0
alpha_shift = 0.05

NZ = 64
HALF = 64
ROWS = HALF + 2 * STEPS
TILES = ROWS // 8
SENT = ROWS - 8
DEEP = STEPS // 2


def tile(t, shift=0):
    return slice(8 + 8 * t + shift, 16 + 8 * t + shift)


def lanes():
    return lax.broadcasted_iota(jnp.int32, (8, 128), 1)


def swap(block):
    return pltpu.roll(block, 64, 1)


def prepare(e_ref, h_ref, c_ref, t_ref, up_ref, down_ref):
    for comp in range(7):
        src, at = ((e_ref, comp) if comp < 3 else (h_ref, comp - 3)) if comp < 6 else (c_ref, 0)
        for j in range(4):
            block = jnp.concatenate(
                [src[at, pl.ds(j, NZ, stride=8), :], src[at, pl.ds(j + 4, NZ, stride=8), :]], 0
            )
            turned = block.T
            up_ref[comp, j] = turned[120:128]
            down_ref[comp, j] = turned[0:8]
            low = lanes() < 64
            for k in range(8):
                first, second = turned[8 * k : 8 * k + 8], turned[64 + 8 * k : 72 + 8 * k]
                t_ref[comp, j, 8 + 8 * k : 16 + 8 * k] = jnp.where(low, first, swap(second))
                t_ref[comp, j + 4, 8 + 8 * k : 16 + 8 * k] = jnp.where(low, swap(first), second)
            before, after = turned[56:64], turned[64:72]
            t_ref[comp, j, 0:8] = swap(before)
            t_ref[comp, j + 4, 0:8] = before
            t_ref[comp, j, 72:80] = after
            t_ref[comp, j + 4, 72:80] = swap(after)


def merge(t_ref, below_ref, above_ref, comp, col, last, write):
    low = lanes() < 64
    for x in range(8):
        for t in range(TILES):
            value = t_ref[comp, x, 8 * t : 8 * t + 8]
            if t == 0:
                halo = below_ref[comp, x % 4]
                halo = swap(halo) if x >= 4 else halo
                value = jnp.where(low, jnp.where(col > 0, halo, 0.0), value)
            if t == TILES - 1:
                halo = above_ref[comp, x % 4]
                halo = swap(halo) if x < 4 else halo
                value = jnp.where(low, value, jnp.where(col < last, halo, 0.0))
            write(x, t, value)


def absorber(positions, total, low, high):
    depth = jnp.maximum(
        jnp.maximum((low - positions) / low, (positions - (total - 1.0 - high)) / high), 0.0
    )
    sigma = sigma_top * depth**3
    damp = jnp.exp(-(sigma + alpha_shift) * time_step)
    gain = sigma / (sigma + alpha_shift) * (damp - 1.0)
    return (damp, gain)


def tables(sc_ref, xt_ref, yt_ref, hc_ref, planes, full_x, full_y):
    widths = [sc_ref[i].astype(jnp.float32) for i in range(4)]
    row, col = sc_ref[4], sc_ref[5]
    for p, x in planes:
        at = jnp.full((8, 128), (row * 8 + x).astype(jnp.float32))
        for k, shift in ((0, 0.5), (2, 0.0)):
            damp, gain = absorber(at + shift, float(full_x), widths[0], widths[1])
            xt_ref[k, p] = damp
            xt_ref[k + 1, p] = gain
    for t in range(TILES):
        half = jnp.where(lanes() < 64, 0, 64)
        y = col * 128 + half + 8 * t - STEPS + lax.broadcasted_iota(jnp.int32, (8, 128), 0)
        at = y.astype(jnp.float32)
        for k, shift in ((0, 0.5), (2, 0.0)):
            damp, gain = absorber(at + shift, float(full_y), widths[2], widths[3])
            yt_ref[k, 8 * t : 8 * t + 8] = damp
            yt_ref[k + 1, 8 * t : 8 * t + 8] = gain
        step = jnp.where(y >= 0, time_step, 0.0)
        hc_ref[0, 8 * t : 8 * t + 8] = step
        hc_ref[1, 8 * t : 8 * t + 8] = jnp.where(row > 0, step, 0.0)


def magnetic(f, psi, p, xt, yt, hc, which):
    z_last = (lanes() & 63) == 63
    damp_x, gain_x = xt[0, p], xt[1, p]
    for t in range(TILES):
        here, rows = tile(t), slice(8 * t, 8 * t + 8)
        e_x, e_y, e_z = f[0, p, here], f[1, p, here], f[2, p, here]
        ez_dy = f[2, p, tile(t, 1)] - e_z
        ex_dy = f[0, p, tile(t, 1)] - e_x
        ey_dz = jnp.where(z_last, 0.0, pltpu.roll(e_y, 127, 1)) - e_y
        ex_dz = jnp.where(z_last, 0.0, pltpu.roll(e_x, 127, 1)) - e_x
        ez_dx = f[2, p + 1, here] - e_z
        ey_dx = f[1, p + 1, here] - e_y
        damp_y, gain_y, step = yt[0, rows], yt[1, rows], hc[which, rows]
        psi_hxy = damp_y * psi[0, p, rows] + gain_y * ez_dy
        psi_hyx = damp_x * psi[1, p, rows] + gain_x * ez_dx
        psi_hzx = damp_x * psi[2, p, rows] + gain_x * ey_dx
        psi_hzy = damp_y * psi[3, p, rows] + gain_y * ex_dy
        psi[0, p, rows] = psi_hxy
        psi[1, p, rows] = psi_hyx
        psi[2, p, rows] = psi_hzx
        psi[3, p, rows] = psi_hzy
        f[3, p, here] = f[3, p, here] - step * (ez_dy + psi_hxy - ey_dz)
        f[4, p, here] = f[4, p, here] - step * (ex_dz - ez_dx - psi_hyx)
        f[5, p, here] = f[5, p, here] - step * (ey_dx + psi_hzx - ex_dy - psi_hzy)


def electric(f, psi, coef, p, xt, yt):
    z_first = (lanes() & 63) == 0
    damp_x, gain_x = xt[2, p], xt[3, p]
    for t in range(TILES):
        here, rows = tile(t), slice(8 * t, 8 * t + 8)
        h_x, h_y, h_z = f[3, p, here], f[4, p, here], f[5, p, here]
        hz_dy = h_z - f[5, p, tile(t, -1)]
        hx_dy = h_x - f[3, p, tile(t, -1)]
        hy_dz = h_y - jnp.where(z_first, 0.0, pltpu.roll(h_y, 1, 1))
        hx_dz = h_x - jnp.where(z_first, 0.0, pltpu.roll(h_x, 1, 1))
        hz_dx = h_z - f[5, p - 1, here]
        hy_dx = h_y - f[4, p - 1, here]
        damp_y, gain_y, step = yt[2, rows], yt[3, rows], coef[p, rows]
        psi_exy = damp_y * psi[4, p, rows] + gain_y * hz_dy
        psi_eyx = damp_x * psi[5, p, rows] + gain_x * hz_dx
        psi_ezx = damp_x * psi[6, p, rows] + gain_x * hy_dx
        psi_ezy = damp_y * psi[7, p, rows] + gain_y * hx_dy
        psi[4, p, rows] = psi_exy
        psi[5, p, rows] = psi_eyx
        psi[6, p, rows] = psi_ezx
        psi[7, p, rows] = psi_ezy
        f[0, p, here] = f[0, p, here] + step * (hz_dy + psi_exy - hy_dz)
        f[1, p, here] = f[1, p, here] + step * (hx_dz - hz_dx - psi_eyx)
        f[2, p, here] = f[2, p, here] + step * (hy_dx + psi_ezx - hx_dy - psi_ezy)


def pack(read, out_ref, at):
    low = lanes() < 64
    for t in range(TILES - 1):
        out_ref[at, 8 * t : 8 * t + 8] = jnp.where(low, read(t), read(t + 1))


def unpack(ref, at, t):
    low = lanes() < 64
    first = ref[at, 8 * t : 8 * t + 8] if t < TILES - 1 else swap(ref[at, 0:8])
    second = ref[at, 8 * t - 8 : 8 * t] if t > 0 else swap(ref[at, SENT - 8 : SENT])
    return jnp.where(low, first, second)


def zero_planes(ref, comps, planes, rows):
    zero = jnp.zeros((rows, 128), jnp.float32)

    def one(p, carry):
        for c in comps:
            ref[c, p] = zero
        return carry

    lax.fori_loop(planes[0], planes[1], one, 0)


def alone(full_x, full_y, last, sc, t_ref, below, above, up_ref, down_ref, f, psi, coef, xt, yt, hc):
    col = sc[5]
    tables(sc, xt, yt, hc, [(1 + x, x) for x in range(8)], full_x, full_y)
    zero_planes(f, range(6), (0, 10), ROWS + 16)
    zero_planes(psi, range(8), (1, 9), ROWS)
    for comp in range(6):

        def write(x, t, value, comp=comp):
            f[comp, 1 + x, tile(t)] = value

        merge(t_ref, below, above, comp, col, last, write)

    def write_coef(x, t, value):
        coef[1 + x, 8 * t : 8 * t + 8] = value

    merge(t_ref, below, above, 6, col, last, write_coef)
    for k in range(DEEP):
        pack(lambda t: coef[5 + k, 8 * t : 8 * t + 8], up_ref, 2 * STEPS + k)
        pack(lambda t: coef[1 + k, 8 * t : 8 * t + 8], down_ref, 2 * STEPS + k)

    def step(s, carry):
        for c in range(2):
            pack(lambda t: f[1 + c, 1, tile(t)], down_ref, 2 * s + c)

        def h_pair(i, carry):
            for k in range(4):
                magnetic(f, psi, 1 + 4 * i + k, xt, yt, hc, 0)
            return carry

        def e_pair(i, carry):
            for k in range(4):
                electric(f, psi, coef, 1 + 4 * i + k, xt, yt)
            return carry

        lax.fori_loop(0, 2, h_pair, 0)
        for c in range(2):
            pack(lambda t: f[4 + c, 8, tile(t)], up_ref, 2 * s + c)
        lax.fori_loop(0, 2, e_pair, 0)
        return carry

    lax.fori_loop(0, STEPS, step, 0)


def joined(
    full_x, full_y, last_row, last, count, sc, snap, t_ref, below, above, left_ref, right_ref, modes_ref,
    out_ref, e_out, h_out, f, psi, coef, xt, yt, hc, planes, snaps, gram_ref, sems,
):
    row, col = sc[4], sc[5]
    cells = [(1 + k, k - 4) for k in range(4)] + [(6 + x, x) for x in range(8)]
    cells = cells + [(15 + k, 8 + k) for k in range(4)]
    tables(sc, xt, yt, hc, cells, full_x, full_y)
    zero_planes(f, range(6), (0, 20), ROWS + 16)
    zero_planes(psi, range(8), (1, 19), ROWS)
    for comp in range(6):

        def write(x, t, value, comp=comp):
            f[comp, 6 + x, tile(t)] = value

        merge(t_ref, below, above, comp, col, last, write)

    def write_coef(x, t, value):
        coef[6 + x, 8 * t : 8 * t + 8] = value

    merge(t_ref, below, above, 6, col, last, write_coef)
    for k in range(DEEP):
        for t in range(TILES):
            rows = slice(8 * t, 8 * t + 8)
            coef[1 + k, rows] = jnp.where(row > 0, unpack(left_ref, 2 * STEPS + k, t), 0.0)
            coef[15 + k, rows] = jnp.where(row < last_row, unpack(right_ref, 2 * STEPS + k, t), 0.0)

    def step(s, carry):
        deep = jnp.minimum(s + 1, STEPS - s)
        for c in range(2):
            for t in range(TILES):
                here = tile(t)
                came = jnp.where(row < last_row, unpack(right_ref, 2 * s + c, t), 0.0)
                f[1 + c, 14, here] = f[1 + c, 15, here] + came
                f[1 + c, 5, here] = f[1 + c, 6, here]

        def h_main(i, carry):
            for k in range(4):
                magnetic(f, psi, 6 + 4 * i + k, xt, yt, hc, 0)
            return carry

        def h_side(k, carry):
            magnetic(f, psi, 4 - k, xt, yt, hc, 1)
            magnetic(f, psi, 15 + k, xt, yt, hc, 0)
            return carry

        def e_main(i, carry):
            for k in range(4):
                electric(f, psi, coef, 6 + 4 * i + k, xt, yt)
            return carry

        def e_side(k, carry):
            electric(f, psi, coef, 4 - k, xt, yt)
            electric(f, psi, coef, 15 + k, xt, yt)
            return carry

        lax.fori_loop(0, 2, h_main, 0)
        lax.fori_loop(0, deep, h_side, 0)
        for c in range(2):
            for t in range(TILES):
                here = tile(t)
                came = jnp.where(row > 0, unpack(left_ref, 2 * s + c, t), 0.0)
                f[4 + c, 5, here] = f[4 + c, 4, here] + came
                f[4 + c, 14, here] = f[4 + c, 13, here]
        lax.fori_loop(0, 2, e_main, 0)
        lax.fori_loop(0, deep, e_side, 0)
        return carry

    lax.fori_loop(0, STEPS, step, 0)

    low = lax.broadcasted_iota(jnp.int32, (HALF, 128), 1) < 64
    own = slice(8 + STEPS, 8 + STEPS + HALF)
    for comp in range(6):
        for j in range(4):
            first, second = f[comp, 6 + j, own], f[comp, 10 + j, own]
            top = jnp.where(low, first, swap(second))
            bottom = jnp.where(low, swap(first), second)
            turned = jnp.concatenate([top, bottom], 0).T
            planes[pl.ds(comp * 8 * NZ + j, NZ, stride=8), :] = turned[:NZ]
            planes[pl.ds(comp * 8 * NZ + j + 4, NZ, stride=8), :] = turned[NZ:]
    size = 3 * NZ * 8
    copies = [
        pltpu.make_async_copy(planes.at[pl.ds(0, size)], e_out, sems.at[0]),
        pltpu.make_async_copy(planes.at[pl.ds(size, size)], h_out, sems.at[1]),
    ]
    for copy in copies:
        copy.start()
    for s in range(count):
        snaps[8 * s : 8 * s + 8] = planes[pl.ds(pl.multiple_of(snap[s] * 8, 8), 8), :]
    gram = jnp.zeros((count, count), jnp.float32)
    coefficients = jnp.zeros((count, 128), jnp.float32)
    contract = functools.partial(
        lax.dot_general,
        dimension_numbers=(((1,), (1,)), ((), ())),
        precision=lax.Precision.HIGHEST,
        preferred_element_type=jnp.float32,
    )
    for x in range(8):
        part = snaps[pl.ds(x, count, stride=8), :]
        gram = gram + contract(part, part)
        coefficients = coefficients + contract(part, modes_ref[pl.ds(x, 128, stride=8), :])
    gram_ref[...] = jnp.concatenate([gram[:32], gram[32:]], 1) / float(full_x * full_y)
    for b in range(8):
        out_ref[b, 0:8] = coefficients[8 * b : 8 * b + 8]
        out_ref[b, 8:12] = gram_ref[4 * b : 4 * b + 4]
    for copy in copies:
        copy.wait()


def around(block, axis, distance):
    size = lax.axis_size(axis)
    return lax.ppermute(block, axis, [(i, (i + distance) % size) for i in range(size)])


def spread(block, axes, size):
    whole = jnp.broadcast_to(block, (size,) + block.shape)
    return lax.all_to_all(whole, axes, split_axis=0, concat_axis=0, tiled=True)


def f32(*shape):
    return jax.ShapeDtypeStruct(shape, jnp.float32)


def shards(e_field, h_field, e_coef, basis, pml_width, snap_index):
    rows_count, cols_count = lax.axis_size(ROW), lax.axis_size(COL)
    full_x, full_y = 8 * rows_count, 128 * cols_count
    row, col = lax.axis_index(ROW), lax.axis_index(COL)
    count = snap_index.shape[0]
    scalars = jnp.concatenate([pml_width, jnp.stack([row, col]).astype(jnp.int32)])
    vmem = pl.BlockSpec(memory_space=pltpu.VMEM)
    smem = pl.BlockSpec(memory_space=pltpu.SMEM)
    params = pltpu.CompilerParams(vmem_limit_bytes=56 * 1024 * 1024)

    local_modes = lax.all_to_all(basis, ROW, split_axis=1, concat_axis=0, tiled=True)

    turned, up, down = pl.pallas_call(
        prepare,
        out_shape=(f32(7, 8, ROWS, 128), f32(7, 4, 8, 128), f32(7, 4, 8, 128)),
        in_specs=[vmem] * 3,
        out_specs=(vmem,) * 3,
        compiler_params=params,
    )(e_field.reshape(3, 512, 128), h_field.reshape(3, 512, 128), e_coef.reshape(1, 512, 128))
    below, above = around(up, COL, 1), around(down, COL, -1)

    def scratch(planes):
        return [
            pltpu.VMEM((6, planes, ROWS + 16, 128), jnp.float32),
            pltpu.VMEM((8, planes, ROWS, 128), jnp.float32),
            pltpu.VMEM((planes, ROWS, 128), jnp.float32),
            pltpu.VMEM((4, planes, 8, 128), jnp.float32),
            pltpu.VMEM((4, ROWS, 128), jnp.float32),
            pltpu.VMEM((2, ROWS, 128), jnp.float32),
        ]

    sent = f32(2 * STEPS + DEEP, SENT, 128)
    up, down = pl.pallas_call(
        functools.partial(alone, full_x, full_y, cols_count - 1),
        out_shape=(sent, sent),
        in_specs=[smem] + [vmem] * 3,
        out_specs=(vmem,) * 2,
        scratch_shapes=scratch(10),
        compiler_params=params,
    )(scalars, turned, below, above)
    left, right = around(up, ROW, 1), around(down, ROW, -1)

    anywhere = pl.BlockSpec(memory_space=pl.ANY)
    sums, e_final, h_final = pl.pallas_call(
        functools.partial(joined, full_x, full_y, rows_count - 1, cols_count - 1, count),
        out_shape=(f32(8, 12, 128), f32(1536, 128), f32(1536, 128)),
        in_specs=[smem] * 2 + [vmem] * 6,
        out_specs=(vmem, anywhere, anywhere),
        scratch_shapes=scratch(20)
        + [
            pltpu.VMEM((6 * NZ * 8, 128), jnp.float32),
            pltpu.VMEM((count * 8, 128), jnp.float32),
            pltpu.VMEM((32, 128), jnp.float32),
            pltpu.SemaphoreType.DMA((2,)),
        ],
        compiler_params=params,
    )(scalars, snap_index, turned, below, above, left, right, local_modes.reshape(1024, 128))

    part = lax.all_to_all(sums, NEAR, split_axis=0, concat_axis=0, tiled=True).sum(0)
    part = spread(part, FAR, lax.axis_size(FAR)).sum(0)
    whole = spread(part, NEAR, lax.axis_size(NEAR))
    coefficients = whole[:, :8].reshape(count, 128)
    packed = whole[:, 8:].reshape(count // 2, 128)
    gram = jnp.concatenate([packed[:, :64], packed[:, 64:]], 0)
    shape = e_field.shape
    return (e_final.reshape(shape), h_final.reshape(shape), coefficients, gram)


def solution(mesh):
    split = Mesh(mesh.devices.reshape(4, 2, 8, 2, 2), ROW + COL)
    return jax.shard_map(
        shards,
        mesh=split,
        in_specs=(
            P(None, None, ROW, COL),
            P(None, None, ROW, COL),
            P(None, ROW, COL),
            P(ROW, None, COL),
            P(),
            P(),
        ),
        out_specs=(P(None, None, ROW, COL), P(None, None, ROW, COL), P(), P()),
        check_vma=False,
    )
```

```python
import functools

import jax
import jax.numpy as jnp
from jax import lax
from jax.experimental import pallas as pl
from jax.experimental.pallas import tpu as pltpu
from jax.sharding import Mesh
from jax.sharding import PartitionSpec as P

STEPS = 8
ROW = ("row_0", "row_1")
COL = ("col_0", "col_1", "col_2")
NEAR = ("row_1", "col_1", "col_2")
FAR = ("row_0", "col_0")

time_step = 0.5
sigma_top = 4.0
alpha_shift = 0.05

NZ = 64
HALF = 64
ROWS = HALF + 2 * STEPS
TILES = ROWS // 8
SENT = ROWS - 8
DEEP = STEPS // 2


def tile(t, shift=0):
    return slice(8 + 8 * t + shift, 16 + 8 * t + shift)


def lanes():
    return lax.broadcasted_iota(jnp.int32, (8, 128), 1)


def swap(block):
    return pltpu.roll(block, 64, 1)


def prepare(e_hbm, h_hbm, c_hbm, t_hbm, up_ref, down_ref, cup_ref, cdown_ref, src, t_ref, sems):
    comes = []
    for comp in range(7):
        ref, at = ((e_hbm, comp) if comp < 3 else (h_hbm, comp - 3)) if comp < 6 else (c_hbm, 0)
        comes.append(pltpu.make_async_copy(ref.at[at], src.at[comp], sems.at[comp]))
        comes[comp].start()
    goes = []
    for comp in range(7):
        comes[comp].wait()
        for j in range(4):
            block = jnp.concatenate(
                [src[comp, pl.ds(j, NZ, stride=8), :], src[comp, pl.ds(j + 4, NZ, stride=8), :]], 0
            )
            turned = block.T
            up_ref[comp, j] = turned[120:128]
            down_ref[comp, j] = turned[0:8]
            low = lanes() < 64
            for k in range(8):
                first, second = turned[8 * k : 8 * k + 8], turned[64 + 8 * k : 72 + 8 * k]
                first, second = jnp.where(low, first, swap(second)), jnp.where(low, swap(first), second)
                t_ref[comp, j, 8 + 8 * k : 16 + 8 * k] = first
                t_ref[comp, j + 4, 8 + 8 * k : 16 + 8 * k] = second
                if comp == 6:
                    cdown_ref[j, 8 * k : 8 * k + 8] = first
                    cup_ref[j, 8 * k : 8 * k + 8] = second
            before, after = turned[56:64], turned[64:72]
            t_ref[comp, j, 0:8] = swap(before)
            t_ref[comp, j + 4, 0:8] = before
            t_ref[comp, j, 72:80] = after
            t_ref[comp, j + 4, 72:80] = swap(after)
        goes.append(pltpu.make_async_copy(t_ref.at[comp], t_hbm.at[comp], sems.at[7 + comp]))
        goes[comp].start()
    for go in goes:
        go.wait()


def fill(f, coef, t_hbm, below_hbm, above_hbm, halo, sems, first):
    copies = []
    for comp in range(6):
        into = f.at[comp, pl.ds(first, 8), pl.ds(8, ROWS), :]
        copies.append(pltpu.make_async_copy(t_hbm.at[comp], into, sems.at[comp]))
    copies.append(pltpu.make_async_copy(t_hbm.at[6], coef.at[pl.ds(first, 8)], sems.at[6]))
    copies.append(pltpu.make_async_copy(below_hbm, halo.at[0], sems.at[7]))
    copies.append(pltpu.make_async_copy(above_hbm, halo.at[1], sems.at[8]))
    return copies


def merge(f, coef, halo, first, col, last):
    low = lanes() < 64
    for comp in range(7):
        for x in range(8):
            below, above = halo[0, comp, x % 4], halo[1, comp, x % 4]
            below = jnp.where(col > 0, swap(below) if x >= 4 else below, 0.0)
            above = jnp.where(col < last, swap(above) if x < 4 else above, 0.0)
            if comp < 6:
                f[comp, first + x, tile(0)] = jnp.where(low, below, f[comp, first + x, tile(0)])
                f[comp, first + x, tile(TILES - 1)] = jnp.where(low, f[comp, first + x, tile(TILES - 1)], above)
            else:
                coef[first + x, 0:8] = jnp.where(low, below, coef[first + x, 0:8])
                coef[first + x, ROWS - 8 : ROWS] = jnp.where(low, coef[first + x, ROWS - 8 : ROWS], above)


def absorber(positions, total, low, high):
    depth = jnp.maximum(
        jnp.maximum((low - positions) / low, (positions - (total - 1.0 - high)) / high), 0.0
    )
    sigma = sigma_top * depth**3
    damp = jnp.exp(-(sigma + alpha_shift) * time_step)
    gain = sigma / (sigma + alpha_shift) * (damp - 1.0)
    return (damp, gain)


def tables(sc_ref, xt_ref, yt_ref, hc_ref, planes, full_x, full_y):
    widths = [sc_ref[i].astype(jnp.float32) for i in range(4)]
    row, col = sc_ref[4], sc_ref[5]
    for p, x in planes:
        at = jnp.full((8, 128), (row * 8 + x).astype(jnp.float32))
        for k, shift in ((0, 0.5), (2, 0.0)):
            damp, gain = absorber(at + shift, float(full_x), widths[0], widths[1])
            xt_ref[k, p] = damp
            xt_ref[k + 1, p] = gain
    for t in range(TILES):
        half = jnp.where(lanes() < 64, 0, 64)
        y = col * 128 + half + 8 * t - STEPS + lax.broadcasted_iota(jnp.int32, (8, 128), 0)
        at = y.astype(jnp.float32)
        for k, shift in ((0, 0.5), (2, 0.0)):
            damp, gain = absorber(at + shift, float(full_y), widths[2], widths[3])
            yt_ref[k, 8 * t : 8 * t + 8] = damp
            yt_ref[k + 1, 8 * t : 8 * t + 8] = gain
        step = jnp.where(y >= 0, time_step, 0.0)
        hc_ref[0, 8 * t : 8 * t + 8] = step
        hc_ref[1, 8 * t : 8 * t + 8] = jnp.where(row > 0, step, 0.0)


def magnetic(f, psi, p, xt, yt, hc, which):
    z_last = (lanes() & 63) == 63
    damp_x, gain_x = xt[0, p], xt[1, p]
    for t in range(TILES):
        here, rows = tile(t), slice(8 * t, 8 * t + 8)
        e_x, e_y, e_z = f[0, p, here], f[1, p, here], f[2, p, here]
        ez_dy = f[2, p, tile(t, 1)] - e_z
        ex_dy = f[0, p, tile(t, 1)] - e_x
        ey_dz = jnp.where(z_last, 0.0, pltpu.roll(e_y, 127, 1)) - e_y
        ex_dz = jnp.where(z_last, 0.0, pltpu.roll(e_x, 127, 1)) - e_x
        ez_dx = f[2, p + 1, here] - e_z
        ey_dx = f[1, p + 1, here] - e_y
        damp_y, gain_y, step = yt[0, rows], yt[1, rows], hc[which, rows]
        psi_hxy = damp_y * psi[0, p, rows] + gain_y * ez_dy
        psi_hyx = damp_x * psi[1, p, rows] + gain_x * ez_dx
        psi_hzx = damp_x * psi[2, p, rows] + gain_x * ey_dx
        psi_hzy = damp_y * psi[3, p, rows] + gain_y * ex_dy
        psi[0, p, rows] = psi_hxy
        psi[1, p, rows] = psi_hyx
        psi[2, p, rows] = psi_hzx
        psi[3, p, rows] = psi_hzy
        f[3, p, here] = f[3, p, here] - step * (ez_dy + psi_hxy - ey_dz)
        f[4, p, here] = f[4, p, here] - step * (ex_dz - ez_dx - psi_hyx)
        f[5, p, here] = f[5, p, here] - step * (ey_dx + psi_hzx - ex_dy - psi_hzy)


def electric(f, psi, coef, p, xt, yt):
    z_first = (lanes() & 63) == 0
    damp_x, gain_x = xt[2, p], xt[3, p]
    for t in range(TILES):
        here, rows = tile(t), slice(8 * t, 8 * t + 8)
        h_x, h_y, h_z = f[3, p, here], f[4, p, here], f[5, p, here]
        hz_dy = h_z - f[5, p, tile(t, -1)]
        hx_dy = h_x - f[3, p, tile(t, -1)]
        hy_dz = h_y - jnp.where(z_first, 0.0, pltpu.roll(h_y, 1, 1))
        hx_dz = h_x - jnp.where(z_first, 0.0, pltpu.roll(h_x, 1, 1))
        hz_dx = h_z - f[5, p - 1, here]
        hy_dx = h_y - f[4, p - 1, here]
        damp_y, gain_y, step = yt[2, rows], yt[3, rows], coef[p, rows]
        psi_exy = damp_y * psi[4, p, rows] + gain_y * hz_dy
        psi_eyx = damp_x * psi[5, p, rows] + gain_x * hz_dx
        psi_ezx = damp_x * psi[6, p, rows] + gain_x * hy_dx
        psi_ezy = damp_y * psi[7, p, rows] + gain_y * hx_dy
        psi[4, p, rows] = psi_exy
        psi[5, p, rows] = psi_eyx
        psi[6, p, rows] = psi_ezx
        psi[7, p, rows] = psi_ezy
        f[0, p, here] = f[0, p, here] + step * (hz_dy + psi_exy - hy_dz)
        f[1, p, here] = f[1, p, here] + step * (hx_dz - hz_dx - psi_eyx)
        f[2, p, here] = f[2, p, here] + step * (hy_dx + psi_ezx - hx_dy - psi_ezy)


def pack(read, out_ref, at):
    low = lanes() < 64
    for t in range(TILES - 1):
        out_ref[pl.ds(pl.multiple_of(at * SENT + 8 * t, 8), 8), :] = jnp.where(low, read(t), read(t + 1))


def unpack(ref, at, t):
    low = lanes() < 64

    def get(k):
        return ref[pl.ds(pl.multiple_of(at * SENT + 8 * k, 8), 8), :]

    first = get(t) if t < TILES - 1 else swap(get(0))
    second = get(t - 1) if t > 0 else swap(get(TILES - 2))
    return jnp.where(low, first, second)


def zero_planes(ref, comps, planes, rows):
    zero = jnp.zeros((rows, 128), jnp.float32)

    def one(p, carry):
        for c in comps:
            ref[c, p] = zero
        return carry

    lax.fori_loop(planes[0], planes[1], one, 0)


def zero_edges(f, first):
    zero = jnp.zeros((8, 128), jnp.float32)
    for comp in range(6):
        for x in range(8):
            f[comp, first + x, 0:8] = zero
            f[comp, first + x, ROWS + 8 : ROWS + 16] = zero


def groups(number, body):
    for i in range(2):
        if isinstance(number, int):
            body(i)
        else:
            pl.when(i < number)(functools.partial(body, i))


def alone(full_x, full_y, last, begin, end, sc, t_hbm, below_hbm, above_hbm, *rest):
    up_ref, down_ref, f, psi, coef, xt, yt, hc, halo, sems = rest
    col = sc[5]
    copies = fill(f, coef, t_hbm, below_hbm, above_hbm, halo, sems, 1)
    for copy in copies:
        copy.start()
    tables(sc, xt, yt, hc, [(1 + x, x) for x in range(8)], full_x, full_y)
    zero_planes(psi, range(8), (1, 9), ROWS)
    zero_planes(f, range(6), (0, 1), ROWS + 16)
    zero_planes(f, range(6), (9, 10), ROWS + 16)
    zero_edges(f, 1)
    for copy in copies:
        copy.wait()
    merge(f, coef, halo, 1, col, last)
    if begin == 0:
        low = lanes() < 64
        for k in range(DEEP):
            at = 2 * end * SENT + 8 * k
            up_ref[at : at + 8] = jnp.where(low, coef[5 + k, 0:8], coef[5 + k, ROWS - 8 : ROWS])
            down_ref[at : at + 8] = jnp.where(low, coef[1 + k, 0:8], coef[1 + k, ROWS - 8 : ROWS])

    def step(s, carry):
        @pl.when(s >= begin)
        def _():
            for c in range(2):
                pack(lambda t: f[1 + c, 1, tile(t)], down_ref, 2 * (s - begin) + c)

        def h_four(i):
            for x in (2 * i, 2 * i + 1, 7 - 2 * i, 6 - 2 * i):
                magnetic(f, psi, 1 + x, xt, yt, hc, 0)

        def e_four(i):
            for x in (2 * i, 2 * i + 1, 7 - 2 * i, 6 - 2 * i):
                electric(f, psi, coef, 1 + x, xt, yt)

        reach = jnp.minimum(4, end - s)
        groups((reach + 1) // 2, h_four)

        @pl.when(s >= begin)
        def _():
            for c in range(2):
                pack(lambda t: f[4 + c, 8, tile(t)], up_ref, 2 * (s - begin) + c)

        reach = jnp.minimum(4, end - 1 - s)
        groups((reach + 1) // 2, e_four)
        return carry

    lax.fori_loop(0, end, step, 0)


CELLS = [(1 + k, k - 4) for k in range(4)] + [(6 + x, x) for x in range(8)] + [(15 + k, 8 + k) for k in range(4)]


def before_magnetic(f, came):
    for c in range(2):
        for t in range(TILES):
            here = tile(t)
            f[1 + c, 14, here] = f[1 + c, 15, here] + came(c, t)
            f[1 + c, 5, here] = f[1 + c, 6, here]


def before_electric(f, came):
    for c in range(2):
        for t in range(TILES):
            here = tile(t)
            f[4 + c, 5, here] = f[4 + c, 4, here] + came(c, t)
            f[4 + c, 14, here] = f[4 + c, 13, here]


def h_side(f, psi, xt, yt, hc):
    def body(i):
        for k in (2 * i, 2 * i + 1):
            magnetic(f, psi, 4 - k, xt, yt, hc, 1)
            magnetic(f, psi, 15 + k, xt, yt, hc, 0)

    return body


def e_side(f, psi, coef, xt, yt):
    def body(i):
        for k in (2 * i, 2 * i + 1):
            electric(f, psi, coef, 4 - k, xt, yt)
            electric(f, psi, coef, 15 + k, xt, yt)

    return body


def h_own(f, psi, xt, yt, hc):
    def body(i):
        for x in (2 * i, 2 * i + 1, 7 - 2 * i, 6 - 2 * i):
            magnetic(f, psi, 6 + x, xt, yt, hc, 0)

    return body


def e_own(f, psi, coef, xt, yt):
    def body(i):
        for x in (2 * i, 2 * i + 1, 7 - 2 * i, 6 - 2 * i):
            electric(f, psi, coef, 6 + x, xt, yt)

    return body


def joined(
    full_x, full_y, last_row, last, early, sc, t_hbm, below_hbm, above_hbm, left_ref, right_ref, cleft_ref,
    cright_ref, end_hbm, f, psi, coef, xt, yt, hc, halo, sems,
):
    row, col = sc[4], sc[5]
    copies = fill(f, coef, t_hbm, below_hbm, above_hbm, halo, sems, 6)
    for copy in copies:
        copy.start()
    tables(sc, xt, yt, hc, CELLS, full_x, full_y)
    zero_planes(psi, range(8), (1, 19), ROWS)
    zero_planes(f, range(6), (0, 6), ROWS + 16)
    zero_planes(f, range(6), (14, 20), ROWS + 16)
    zero_edges(f, 6)
    for copy in copies:
        copy.wait()
    merge(f, coef, halo, 6, col, last)
    low = lanes() < 64
    for ref, edge_ref, first, there in (
        (cleft_ref, left_ref, 1, row > 0),
        (cright_ref, right_ref, 15, row < last_row),
    ):
        for k in range(DEEP):
            at = 2 * early * SENT + 8 * k
            corner = edge_ref[at : at + 8]
            for t in range(TILES):
                if t == 0:
                    value = jnp.where(low, corner, swap(ref[k, HALF - 8 : HALF]))
                elif t == TILES - 1:
                    value = jnp.where(low, swap(ref[k, 0:8]), corner)
                else:
                    value = ref[k, 8 * t - 8 : 8 * t]
                coef[first + k, 8 * t : 8 * t + 8] = jnp.where(there, value, 0.0)

    out = pltpu.make_async_copy(coef, end_hbm.at[pl.ds(48, 20)], sems.at[6])
    out.start()

    def step(s, carry):
        deep = jnp.minimum(s + 1, STEPS - s)
        at = 2 * jnp.minimum(s, early - 1)
        from_above = jnp.logical_and(row < last_row, s < early)
        from_below = jnp.logical_and(row > 0, s < early)
        before_magnetic(f, lambda c, t: jnp.where(from_above, unpack(right_ref, at + c, t), 0.0))
        groups(2, h_own(f, psi, xt, yt, hc))
        groups((deep + 1) // 2, h_side(f, psi, xt, yt, hc))
        before_electric(f, lambda c, t: jnp.where(from_below, unpack(left_ref, at + c, t), 0.0))
        groups(2, e_own(f, psi, coef, xt, yt))
        groups((deep + 1) // 2, e_side(f, psi, coef, xt, yt))
        return carry

    lax.fori_loop(0, STEPS, step, 0)
    out.wait()
    outs = []
    for comp in range(6):
        own = f.at[comp, pl.ds(6, 8), pl.ds(8, ROWS), :]
        outs.append(pltpu.make_async_copy(own, end_hbm.at[pl.ds(8 * comp, 8)], sems.at[comp]))
        outs[comp].start()
    for copy in outs:
        copy.wait()


def late(
    full_x, full_y, last_row, early, count, sc, snap, end_hbm, left_ref, right_ref, modes_hbm,
    out_ref, e_out, h_out, f, psi, coef, xt, yt, hc, end_ref, modes_ref, planes, snaps, gram_ref, sems,
):
    row = sc[4]
    coef_in = pltpu.make_async_copy(end_hbm.at[pl.ds(48, 20)], coef, sems.at[2])
    end_in = pltpu.make_async_copy(end_hbm.at[pl.ds(0, 48)], end_ref, sems.at[3])
    modes_in = pltpu.make_async_copy(modes_hbm, modes_ref, sems.at[4])
    for copy in (coef_in, end_in, modes_in):
        copy.start()
    tables(sc, xt, yt, hc, CELLS, full_x, full_y)
    zero_planes(f, range(6), (2, 18), ROWS + 16)
    zero_planes(psi, range(8), (3, 17), ROWS)
    coef_in.wait()
    count_late = STEPS - early

    def step(j, carry):
        deep = jnp.minimum(j + 1, count_late - j)
        reach = jnp.minimum(j + 1, 4)
        before_magnetic(f, lambda c, t: jnp.where(row < last_row, unpack(right_ref, 2 * j + c, t), 0.0))
        groups((reach + 1) // 2, h_own(f, psi, xt, yt, hc))
        groups((deep + 1) // 2, h_side(f, psi, xt, yt, hc))
        before_electric(f, lambda c, t: jnp.where(row > 0, unpack(left_ref, 2 * j + c, t), 0.0))
        groups((reach + 1) // 2, e_own(f, psi, coef, xt, yt))
        groups((deep + 1) // 2, e_side(f, psi, coef, xt, yt))
        return carry

    lax.fori_loop(0, count_late, step, 0)
    end_in.wait()

    low = lax.broadcasted_iota(jnp.int32, (HALF, 128), 1) < 64
    own = slice(8 + STEPS, 8 + STEPS + HALF)
    for comp in range(6):
        for j in range(4):
            first = f[comp, 6 + j, own] + end_ref[8 * comp + j, STEPS : STEPS + HALF]
            second = f[comp, 10 + j, own] + end_ref[8 * comp + 4 + j, STEPS : STEPS + HALF]
            top = jnp.where(low, first, swap(second))
            bottom = jnp.where(low, swap(first), second)
            turned = jnp.concatenate([top, bottom], 0).T
            planes[pl.ds(comp * 8 * NZ + j, NZ, stride=8), :] = turned[:NZ]
            planes[pl.ds(comp * 8 * NZ + j + 4, NZ, stride=8), :] = turned[NZ:]
    size = 3 * NZ * 8
    copies = [
        pltpu.make_async_copy(planes.at[pl.ds(0, size)], e_out, sems.at[0]),
        pltpu.make_async_copy(planes.at[pl.ds(size, size)], h_out, sems.at[1]),
    ]
    for copy in copies:
        copy.start()
    modes_in.wait()
    for s in range(count):
        snaps[8 * s : 8 * s + 8] = planes[pl.ds(pl.multiple_of(snap[s] * 8, 8), 8), :]
    gram = jnp.zeros((count, count), jnp.float32)
    coefficients = jnp.zeros((count, 128), jnp.float32)
    contract = functools.partial(
        lax.dot_general,
        dimension_numbers=(((1,), (1,)), ((), ())),
        precision=lax.Precision.HIGHEST,
        preferred_element_type=jnp.float32,
    )
    for x in range(8):
        part = snaps[pl.ds(x, count, stride=8), :]
        gram = gram + contract(part, part)
        coefficients = coefficients + contract(part, modes_ref[pl.ds(x, 128, stride=8), :])
    gram_ref[...] = jnp.concatenate([gram[:32], gram[32:]], 1) / float(full_x * full_y)
    for b in range(8):
        out_ref[b, 0:8] = coefficients[8 * b : 8 * b + 8]
        out_ref[b, 8:12] = gram_ref[4 * b : 4 * b + 4]
    for copy in copies:
        copy.wait()


def around(block, axis, distance):
    size = lax.axis_size(axis)
    return lax.ppermute(block, axis, [(i, (i + distance) % size) for i in range(size)])


def spread(block, axes, size):
    whole = jnp.broadcast_to(block, (size,) + block.shape)
    return lax.all_to_all(whole, axes, split_axis=0, concat_axis=0, tiled=True)


def f32(*shape):
    return jax.ShapeDtypeStruct(shape, jnp.float32)


def call(kernel, flops, limit, **kwargs):
    return pl.pallas_call(
        kernel,
        compiler_params=pltpu.CompilerParams(vmem_limit_bytes=limit * 1024 * 1024),
        cost_estimate=pl.CostEstimate(flops=flops, bytes_accessed=4_000_000, transcendentals=0),
        **kwargs,
    )


def scratch(planes, *more):
    shapes = [(6, planes, ROWS + 16, 128), (8, planes, ROWS, 128), (planes, ROWS, 128)]
    shapes = shapes + [(4, planes, 8, 128), (4, ROWS, 128), (2, ROWS, 128)] + list(more)
    return [pltpu.VMEM(shape, jnp.float32) for shape in shapes]


HALO = (2, 7, 4, 8, 128)
EARLY = 4


def shards(e_field, h_field, e_coef, basis, pml_width, snap_index):
    rows_count, cols_count = lax.axis_size(ROW), lax.axis_size(COL)
    full_x, full_y = 8 * rows_count, 128 * cols_count
    row, col = lax.axis_index(ROW), lax.axis_index(COL)
    count = snap_index.shape[0]
    scalars = jnp.concatenate([pml_width, jnp.stack([row, col]).astype(jnp.int32)])
    vmem = pl.BlockSpec(memory_space=pltpu.VMEM)
    smem = pl.BlockSpec(memory_space=pltpu.SMEM)
    hbm = pl.BlockSpec(memory_space=pltpu.HBM)

    turned, up, down, c_up, c_down = call(
        prepare, 10**9, PREPARE_MIB,
        out_shape=(f32(7, 8, ROWS, 128),) + (f32(7, 4, 8, 128),) * 2 + (f32(4, HALF, 128),) * 2,
        in_specs=[hbm] * 3,
        out_specs=(hbm,) + (vmem,) * 4,
        scratch_shapes=[
            pltpu.VMEM((7, 512, 128), jnp.float32),
            pltpu.VMEM((7, 8, ROWS, 128), jnp.float32),
            pltpu.SemaphoreType.DMA((14,)),
        ],
    )(e_field.reshape(3, 512, 128), h_field.reshape(3, 512, 128), e_coef.reshape(1, 512, 128))
    below, above = around(up, COL, 1), around(down, COL, -1)
    c_left, c_right = around(c_up, ROW, 1), around(c_down, ROW, -1)

    def run_alone(begin, end):
        sent = f32(2 * (end - begin) * SENT + (8 * DEEP if begin == 0 else 0), 128)
        return call(
            functools.partial(alone, full_x, full_y, cols_count - 1, begin, end), 4 * 10**9, ALONE_MIB,
            out_shape=(sent, sent),
            in_specs=[smem] + [hbm] * 3,
            out_specs=(vmem,) * 2,
            scratch_shapes=scratch(10, HALO) + [pltpu.SemaphoreType.DMA((9,))],
        )(scalars, turned, below, above)

    with jax.named_scope("alone_a"):
        up, down = run_alone(0, EARLY)
    left, right = around(up, ROW, 1), around(down, ROW, -1)
    with jax.named_scope("alone_b"):
        up, down = run_alone(EARLY, STEPS)
    with jax.named_scope("turn"):
        modes, up = lax.optimization_barrier((basis, up))
        modes = modes.reshape(16, rows_count, 8, 128).transpose(1, 0, 2, 3)
        modes = lax.all_to_all(modes, ROW, split_axis=0, concat_axis=0, tiled=True).reshape(1024, 128)
    up, down, left, right = lax.optimization_barrier((up, down, left, right))
    left_late, right_late = around(up, ROW, 1), around(down, ROW, -1)

    with jax.named_scope("joined"):
        ends = call(
            functools.partial(joined, full_x, full_y, rows_count - 1, cols_count - 1, EARLY), 12 * 10**9, JOINED_MIB,
            out_shape=f32(68, ROWS, 128),
            in_specs=[smem] + [hbm] * 3 + [vmem] * 4,
            out_specs=hbm,
            scratch_shapes=scratch(20, HALO) + [pltpu.SemaphoreType.DMA((9,))],
        )(scalars, turned, below, above, left, right, c_left, c_right)

    sums, e_final, h_final = call(
        functools.partial(late, full_x, full_y, rows_count - 1, EARLY, count), 4 * 10**9, LATE_MIB,
        out_shape=(f32(8, 12, 128), f32(1536, 128), f32(1536, 128)),
        in_specs=[smem] * 2 + [hbm] + [vmem] * 2 + [hbm],
        out_specs=(vmem, hbm, hbm),
        scratch_shapes=scratch(20, (48, ROWS, 128), (1024, 128))
        + [
            pltpu.VMEM((6 * NZ * 8, 128), jnp.float32),
            pltpu.VMEM((count * 8, 128), jnp.float32),
            pltpu.VMEM((32, 128), jnp.float32),
            pltpu.SemaphoreType.DMA((5,)),
        ],
    )(scalars, snap_index, ends, left_late, right_late, modes)

    part = lax.all_to_all(sums, NEAR, split_axis=0, concat_axis=0, tiled=True).sum(0)
    part = spread(part, FAR, lax.axis_size(FAR)).sum(0)
    whole = spread(part, NEAR, lax.axis_size(NEAR))
    coefficients = whole[:, :8].reshape(count, 128)
    packed = whole[:, 8:].reshape(count // 2, 128)
    gram = jnp.concatenate([packed[:, :64], packed[:, 64:]], 0)
    shape = e_field.shape
    return (e_final.reshape(shape), h_final.reshape(shape), coefficients, gram)


PREPARE_MIB, ALONE_MIB, JOINED_MIB, LATE_MIB = 56, 60, 60, 60


def solution(mesh):
    split = Mesh(mesh.devices.reshape(4, 2, 8, 2, 2), ROW + COL)
    return jax.shard_map(
        shards,
        mesh=split,
        in_specs=(
            P(None, None, ROW, COL),
            P(None, None, ROW, COL),
            P(None, ROW, COL),
            P(ROW, None, COL),
            P(),
            P(),
        ),
        out_specs=(P(None, None, ROW, COL), P(None, None, ROW, COL), P(), P()),
        check_vma=False,
    )
```

```python
import functools

import jax
import jax.numpy as jnp
from jax import lax
from jax.experimental import pallas as pl
from jax.experimental.pallas import tpu as pltpu
from jax.sharding import Mesh
from jax.sharding import PartitionSpec as P


STEPS = 8
ROW = ("row_0", "row_1")
COL = ("col_0", "col_1", "col_2")
NEAR = ("row_1", "col_1", "col_2")
FAR = ("row_0", "col_0")

time_step = 0.5
sigma_top = 4.0
alpha_shift = 0.05

NZ = 64
HALF = 64
ROWS = HALF + 2 * STEPS
TILES = ROWS // 8
SENT = ROWS - 8
DEEP = STEPS // 2


def tile(t, shift=0):
    return slice(8 + 8 * t + shift, 16 + 8 * t + shift)


def lanes():
    return lax.broadcasted_iota(jnp.int32, (8, 128), 1)


def swap(block):
    return pltpu.roll(block, 64, 1)


def prepare(e_ref, h_ref, c_ref, t_ref, up_ref, down_ref, cup_ref, cdown_ref):
    for comp in range(7):
        src, at = ((e_ref, comp) if comp < 3 else (h_ref, comp - 3)) if comp < 6 else (c_ref, 0)
        for j in range(4):
            block = jnp.concatenate(
                [src[at, pl.ds(j, NZ, stride=8), :], src[at, pl.ds(j + 4, NZ, stride=8), :]], 0
            )
            turned = block.T
            up_ref[comp, j] = turned[120:128]
            down_ref[comp, j] = turned[0:8]
            low = lanes() < 64
            for k in range(8):
                first, second = turned[8 * k : 8 * k + 8], turned[64 + 8 * k : 72 + 8 * k]
                first, second = jnp.where(low, first, swap(second)), jnp.where(low, swap(first), second)
                t_ref[comp, j, 8 + 8 * k : 16 + 8 * k] = first
                t_ref[comp, j + 4, 8 + 8 * k : 16 + 8 * k] = second
                if comp == 6:
                    cdown_ref[j, 8 * k : 8 * k + 8] = first
                    cup_ref[j, 8 * k : 8 * k + 8] = second
            before, after = turned[56:64], turned[64:72]
            t_ref[comp, j, 0:8] = swap(before)
            t_ref[comp, j + 4, 0:8] = before
            t_ref[comp, j, 72:80] = after
            t_ref[comp, j + 4, 72:80] = swap(after)


def fill(f, coef, t_ref, first):
    for x in range(8):
        for t in range(TILES):
            rows = slice(8 * t, 8 * t + 8)
            for comp in range(6):
                f[comp, first + x, tile(t)] = t_ref[comp, x, rows]
            coef[first + x, rows] = t_ref[6, x, rows]


def merge(f, coef, below_ref, above_ref, first, col, last):
    low = lanes() < 64
    for comp in range(7):
        for x in range(8):
            below, above = below_ref[comp, x % 4], above_ref[comp, x % 4]
            below = jnp.where(col > 0, swap(below) if x >= 4 else below, 0.0)
            above = jnp.where(col < last, swap(above) if x < 4 else above, 0.0)
            if comp < 6:
                f[comp, first + x, tile(0)] = jnp.where(low, below, f[comp, first + x, tile(0)])
                f[comp, first + x, tile(TILES - 1)] = jnp.where(low, f[comp, first + x, tile(TILES - 1)], above)
            else:
                coef[first + x, 0:8] = jnp.where(low, below, coef[first + x, 0:8])
                coef[first + x, ROWS - 8 : ROWS] = jnp.where(low, coef[first + x, ROWS - 8 : ROWS], above)


def absorber(positions, total, low, high):
    depth = jnp.maximum(
        jnp.maximum((low - positions) / low, (positions - (total - 1.0 - high)) / high), 0.0
    )
    sigma = sigma_top * depth**3
    damp = jnp.exp(-(sigma + alpha_shift) * time_step)
    gain = sigma / (sigma + alpha_shift) * (damp - 1.0)
    return (damp, gain)


def tables(sc_ref, xt_ref, yt_ref, hc_ref, planes, full_x, full_y):
    widths = [sc_ref[i].astype(jnp.float32) for i in range(4)]
    row, col = lax.axis_index(ROW), lax.axis_index(COL)
    for p, x in planes:
        at = jnp.full((8, 128), (row * 8 + x).astype(jnp.float32))
        for k, shift in ((0, 0.5), (2, 0.0)):
            damp, gain = absorber(at + shift, float(full_x), widths[0], widths[1])
            xt_ref[k, p] = damp
            xt_ref[k + 1, p] = gain
    for t in range(TILES):
        half = jnp.where(lanes() < 64, 0, 64)
        y = col * 128 + half + 8 * t - STEPS + lax.broadcasted_iota(jnp.int32, (8, 128), 0)
        at = y.astype(jnp.float32)
        for k, shift in ((0, 0.5), (2, 0.0)):
            damp, gain = absorber(at + shift, float(full_y), widths[2], widths[3])
            yt_ref[k, 8 * t : 8 * t + 8] = damp
            yt_ref[k + 1, 8 * t : 8 * t + 8] = gain
        step = jnp.where(y >= 0, time_step, 0.0)
        hc_ref[0, 8 * t : 8 * t + 8] = step
        hc_ref[1, 8 * t : 8 * t + 8] = jnp.where(row > 0, step, 0.0)


def magnetic(f, psi, p, xt, yt, hc, which):
    z_last = (lanes() & 63) == 63
    damp_x, gain_x = xt[0, p], xt[1, p]
    for t in range(TILES):
        here, rows = tile(t), slice(8 * t, 8 * t + 8)
        e_x, e_y, e_z = f[0, p, here], f[1, p, here], f[2, p, here]
        ez_dy = f[2, p, tile(t, 1)] - e_z
        ex_dy = f[0, p, tile(t, 1)] - e_x
        ey_dz = jnp.where(z_last, 0.0, pltpu.roll(e_y, 127, 1)) - e_y
        ex_dz = jnp.where(z_last, 0.0, pltpu.roll(e_x, 127, 1)) - e_x
        ez_dx = f[2, p + 1, here] - e_z
        ey_dx = f[1, p + 1, here] - e_y
        damp_y, gain_y, step = yt[0, rows], yt[1, rows], hc[which, rows]
        psi_hxy = damp_y * psi[0, p, rows] + gain_y * ez_dy
        psi_hyx = damp_x * psi[1, p, rows] + gain_x * ez_dx
        psi_hzx = damp_x * psi[2, p, rows] + gain_x * ey_dx
        psi_hzy = damp_y * psi[3, p, rows] + gain_y * ex_dy
        psi[0, p, rows] = psi_hxy
        psi[1, p, rows] = psi_hyx
        psi[2, p, rows] = psi_hzx
        psi[3, p, rows] = psi_hzy
        f[3, p, here] = f[3, p, here] - step * (ez_dy + psi_hxy - ey_dz)
        f[4, p, here] = f[4, p, here] - step * (ex_dz - ez_dx - psi_hyx)
        f[5, p, here] = f[5, p, here] - step * (ey_dx + psi_hzx - ex_dy - psi_hzy)


def electric(f, psi, coef, p, xt, yt):
    z_first = (lanes() & 63) == 0
    damp_x, gain_x = xt[2, p], xt[3, p]
    for t in range(TILES):
        here, rows = tile(t), slice(8 * t, 8 * t + 8)
        h_x, h_y, h_z = f[3, p, here], f[4, p, here], f[5, p, here]
        hz_dy = h_z - f[5, p, tile(t, -1)]
        hx_dy = h_x - f[3, p, tile(t, -1)]
        hy_dz = h_y - jnp.where(z_first, 0.0, pltpu.roll(h_y, 1, 1))
        hx_dz = h_x - jnp.where(z_first, 0.0, pltpu.roll(h_x, 1, 1))
        hz_dx = h_z - f[5, p - 1, here]
        hy_dx = h_y - f[4, p - 1, here]
        damp_y, gain_y, step = yt[2, rows], yt[3, rows], coef[p, rows]
        psi_exy = damp_y * psi[4, p, rows] + gain_y * hz_dy
        psi_eyx = damp_x * psi[5, p, rows] + gain_x * hz_dx
        psi_ezx = damp_x * psi[6, p, rows] + gain_x * hy_dx
        psi_ezy = damp_y * psi[7, p, rows] + gain_y * hx_dy
        psi[4, p, rows] = psi_exy
        psi[5, p, rows] = psi_eyx
        psi[6, p, rows] = psi_ezx
        psi[7, p, rows] = psi_ezy
        f[0, p, here] = f[0, p, here] + step * (hz_dy + psi_exy - hy_dz)
        f[1, p, here] = f[1, p, here] + step * (hx_dz - hz_dx - psi_eyx)
        f[2, p, here] = f[2, p, here] + step * (hy_dx + psi_ezx - hx_dy - psi_ezy)


def pack(read, out_ref, at):
    low = lanes() < 64
    for t in range(TILES - 1):
        out_ref[pl.ds(pl.multiple_of(at * SENT + 8 * t, 8), 8), :] = jnp.where(low, read(t), read(t + 1))


def unpack(ref, at, t):
    low = lanes() < 64

    def get(k):
        return ref[pl.ds(pl.multiple_of(at * SENT + 8 * k, 8), 8), :]

    first = get(t) if t < TILES - 1 else swap(get(0))
    second = get(t - 1) if t > 0 else swap(get(TILES - 2))
    return jnp.where(low, first, second)


def zero_planes(ref, comps, planes, rows):
    zero = jnp.zeros((rows, 128), jnp.float32)

    def one(p, carry):
        for c in comps:
            ref[c, p] = zero
        return carry

    lax.fori_loop(planes[0], planes[1], one, 0)


def zero_edges(f, first):
    zero = jnp.zeros((8, 128), jnp.float32)
    for comp in range(6):
        for x in range(8):
            f[comp, first + x, 0:8] = zero
            f[comp, first + x, ROWS + 8 : ROWS + 16] = zero


def groups(number, body):
    for i in range(2):
        if isinstance(number, int):
            body(i)
        else:
            pl.when(i < number)(functools.partial(body, i))


def alone(full_x, full_y, last, begin, end, sc, t_ref, below_ref, above_ref, *rest):
    col = lax.axis_index(COL)
    if begin > 0:
        (keep_ref, up_ref, down_ref), scratches = rest[:3], rest[3:]
        for comp in range(7):
            keep_ref[comp] = t_ref[comp]
    else:
        (up_ref, down_ref), scratches = rest[:2], rest[2:]
    f, psi, coef, xt, yt, hc = scratches
    fill(f, coef, t_ref, 1)
    tables(sc, xt, yt, hc, [(1 + x, x) for x in range(8)], full_x, full_y)
    zero_planes(psi, range(8), (1, 9), ROWS)
    zero_planes(f, range(6), (0, 1), ROWS + 16)
    zero_planes(f, range(6), (9, 10), ROWS + 16)
    zero_edges(f, 1)
    merge(f, coef, below_ref, above_ref, 1, col, last)
    if begin == 0:
        low = lanes() < 64
        for k in range(DEEP):
            at = 2 * end * SENT + 8 * k
            up_ref[at : at + 8] = jnp.where(low, coef[5 + k, 0:8], coef[5 + k, ROWS - 8 : ROWS])
            down_ref[at : at + 8] = jnp.where(low, coef[1 + k, 0:8], coef[1 + k, ROWS - 8 : ROWS])

    def step(s, carry):
        @pl.when(s >= begin)
        def _():
            for c in range(2):
                pack(lambda t: f[1 + c, 1, tile(t)], down_ref, 2 * (s - begin) + c)

        def h_four(i):
            for x in (2 * i, 2 * i + 1, 7 - 2 * i, 6 - 2 * i):
                magnetic(f, psi, 1 + x, xt, yt, hc, 0)

        def e_four(i):
            for x in (2 * i, 2 * i + 1, 7 - 2 * i, 6 - 2 * i):
                electric(f, psi, coef, 1 + x, xt, yt)

        reach = jnp.minimum(4, end - s)
        groups((reach + 1) // 2, h_four)

        @pl.when(s >= begin)
        def _():
            for c in range(2):
                pack(lambda t: f[4 + c, 8, tile(t)], up_ref, 2 * (s - begin) + c)

        reach = jnp.minimum(4, end - 1 - s)
        groups((reach + 1) // 2, e_four)
        return carry

    lax.fori_loop(0, end, step, 0)


CELLS = [(1 + k, k - 4) for k in range(4)] + [(6 + x, x) for x in range(8)] + [(15 + k, 8 + k) for k in range(4)]


def before_magnetic(f, came):
    for c in range(2):
        for t in range(TILES):
            here = tile(t)
            f[1 + c, 14, here] = f[1 + c, 15, here] + came(c, t)
            f[1 + c, 5, here] = f[1 + c, 6, here]


def before_electric(f, came):
    for c in range(2):
        for t in range(TILES):
            here = tile(t)
            f[4 + c, 5, here] = f[4 + c, 4, here] + came(c, t)
            f[4 + c, 14, here] = f[4 + c, 13, here]


def h_side(f, psi, xt, yt, hc):
    def body(i):
        for k in (2 * i, 2 * i + 1):
            magnetic(f, psi, 4 - k, xt, yt, hc, 1)
            magnetic(f, psi, 15 + k, xt, yt, hc, 0)

    return body


def e_side(f, psi, coef, xt, yt):
    def body(i):
        for k in (2 * i, 2 * i + 1):
            electric(f, psi, coef, 4 - k, xt, yt)
            electric(f, psi, coef, 15 + k, xt, yt)

    return body


def h_own(f, psi, xt, yt, hc):
    def body(i):
        for x in (2 * i, 2 * i + 1, 7 - 2 * i, 6 - 2 * i):
            magnetic(f, psi, 6 + x, xt, yt, hc, 0)

    return body


def e_own(f, psi, coef, xt, yt):
    def body(i):
        for x in (2 * i, 2 * i + 1, 7 - 2 * i, 6 - 2 * i):
            electric(f, psi, coef, 6 + x, xt, yt)

    return body


def joined(
    full_x, full_y, last_row, last, early, sc, t_ref, below_ref, above_ref, left_ref, right_ref, cleft_ref,
    cright_ref, end_ref, f, psi, xt, yt, hc,
):
    row, col = lax.axis_index(ROW), lax.axis_index(COL)
    coef = end_ref.at[pl.ds(48, 20)]
    fill(f, coef, t_ref, 6)
    tables(sc, xt, yt, hc, CELLS, full_x, full_y)
    zero_planes(psi, range(8), (1, 19), ROWS)
    zero_planes(f, range(6), (0, 6), ROWS + 16)
    zero_planes(f, range(6), (14, 20), ROWS + 16)
    zero_edges(f, 6)
    merge(f, coef, below_ref, above_ref, 6, col, last)
    low = lanes() < 64
    for ref, edge_ref, first, there in (
        (cleft_ref, left_ref, 1, row > 0),
        (cright_ref, right_ref, 15, row < last_row),
    ):
        for k in range(DEEP):
            at = 2 * early * SENT + 8 * k
            corner = edge_ref[at : at + 8]
            for t in range(TILES):
                if t == 0:
                    value = jnp.where(low, corner, swap(ref[k, HALF - 8 : HALF]))
                elif t == TILES - 1:
                    value = jnp.where(low, swap(ref[k, 0:8]), corner)
                else:
                    value = ref[k, 8 * t - 8 : 8 * t]
                coef[first + k, 8 * t : 8 * t + 8] = jnp.where(there, value, 0.0)

    def step(s, carry):
        deep = jnp.minimum(s + 1, STEPS - s)
        at = 2 * jnp.minimum(s, early - 1)
        from_above = jnp.logical_and(row < last_row, s < early)
        from_below = jnp.logical_and(row > 0, s < early)
        before_magnetic(f, lambda c, t: jnp.where(from_above, unpack(right_ref, at + c, t), 0.0))
        groups(2, h_own(f, psi, xt, yt, hc))
        groups((deep + 1) // 2, h_side(f, psi, xt, yt, hc))
        before_electric(f, lambda c, t: jnp.where(from_below, unpack(left_ref, at + c, t), 0.0))
        groups(2, e_own(f, psi, coef, xt, yt))
        groups((deep + 1) // 2, e_side(f, psi, coef, xt, yt))
        return carry

    lax.fori_loop(0, STEPS, step, 0)
    for comp in range(6):
        for x in range(8):
            end_ref[8 * comp + x, STEPS : STEPS + HALF] = f[comp, 6 + x, 8 + STEPS : 8 + STEPS + HALF]


def late(
    full_x, full_y, last_row, early, count, sc, snap, end_ref, left_ref, right_ref, modes_ref,
    out_ref, e_out, h_out, f, psi, xt, yt, hc, planes, snaps, gram_ref, sems,
):
    row = lax.axis_index(ROW)
    coef = end_ref.at[pl.ds(48, 20)]
    tables(sc, xt, yt, hc, CELLS, full_x, full_y)
    zero_planes(f, range(6), (2, 18), ROWS + 16)
    zero_planes(psi, range(8), (3, 17), ROWS)
    count_late = STEPS - early

    def step(j, carry):
        deep = jnp.minimum(j + 1, count_late - j)
        reach = jnp.minimum(j + 1, 4)
        before_magnetic(f, lambda c, t: jnp.where(row < last_row, unpack(right_ref, 2 * j + c, t), 0.0))
        groups((reach + 1) // 2, h_own(f, psi, xt, yt, hc))
        groups((deep + 1) // 2, h_side(f, psi, xt, yt, hc))
        before_electric(f, lambda c, t: jnp.where(row > 0, unpack(left_ref, 2 * j + c, t), 0.0))
        groups((reach + 1) // 2, e_own(f, psi, coef, xt, yt))
        groups((deep + 1) // 2, e_side(f, psi, coef, xt, yt))
        return carry

    lax.fori_loop(0, count_late, step, 0)

    low = lax.broadcasted_iota(jnp.int32, (HALF, 128), 1) < 64
    own = slice(8 + STEPS, 8 + STEPS + HALF)
    for comp in range(6):
        for j in range(4):
            first = f[comp, 6 + j, own] + end_ref[8 * comp + j, STEPS : STEPS + HALF]
            second = f[comp, 10 + j, own] + end_ref[8 * comp + 4 + j, STEPS : STEPS + HALF]
            top = jnp.where(low, first, swap(second))
            bottom = jnp.where(low, swap(first), second)
            turned = jnp.concatenate([top, bottom], 0).T
            planes[pl.ds(comp * 8 * NZ + j, NZ, stride=8), :] = turned[:NZ]
            planes[pl.ds(comp * 8 * NZ + j + 4, NZ, stride=8), :] = turned[NZ:]
    size = 3 * NZ * 8
    copies = [
        pltpu.make_async_copy(planes.at[pl.ds(0, size)], e_out, sems.at[0]),
        pltpu.make_async_copy(planes.at[pl.ds(size, size)], h_out, sems.at[1]),
    ]
    for copy in copies:
        copy.start()
    for s in range(count):
        snaps[8 * s : 8 * s + 8] = planes[pl.ds(pl.multiple_of(snap[s] * 8, 8), 8), :]
    gram = jnp.zeros((count, count), jnp.float32)
    coefficients = jnp.zeros((count, 128), jnp.float32)
    contract = functools.partial(
        lax.dot_general,
        dimension_numbers=(((1,), (1,)), ((), ())),
        precision=lax.Precision.HIGHEST,
        preferred_element_type=jnp.float32,
    )
    for x in range(8):
        part = snaps[pl.ds(x, count, stride=8), :]
        gram = gram + contract(part, part)
        coefficients = coefficients + contract(part, modes_ref[pl.ds(x, 128, stride=8), :])
    gram_ref[...] = jnp.concatenate([gram[:32], gram[32:]], 1) / float(full_x * full_y)
    for b in range(8):
        out_ref[b, 0:8] = coefficients[8 * b : 8 * b + 8]
        out_ref[b, 8:12] = gram_ref[4 * b : 4 * b + 4]
    for copy in copies:
        copy.wait()


def part_out(whole_ref, coef_ref, gram_ref):
    for b in range(8):
        coef_ref[8 * b : 8 * b + 8] = whole_ref[b, 0:8]
        packed = whole_ref[b, 8:12]
        gram_ref[4 * b : 4 * b + 4] = packed[:, :64]
        gram_ref[32 + 4 * b : 36 + 4 * b] = packed[:, 64:]


def around(block, axis, distance):
    size = lax.axis_size(axis)
    return lax.ppermute(block, axis, [(i, (i + distance) % size) for i in range(size)])


def spread(block, axes, size):
    whole = jnp.broadcast_to(block, (size,) + block.shape)
    return lax.all_to_all(whole, axes, split_axis=0, concat_axis=0, tiled=True)


def f32(*shape):
    return jax.ShapeDtypeStruct(shape, jnp.float32)


def call(kernel, flops, limit, **kwargs):
    return pl.pallas_call(
        kernel,
        compiler_params=pltpu.CompilerParams(vmem_limit_bytes=limit * 1024 * 1024),
        cost_estimate=pl.CostEstimate(flops=flops, bytes_accessed=4_000_000, transcendentals=0),
        **kwargs,
    )


def scratch(planes, coef):
    shapes = [(6, planes, ROWS + 16, 128), (8, planes, ROWS, 128)] + [(planes, ROWS, 128)] * coef
    shapes = shapes + [(4, planes, 8, 128), (4, ROWS, 128), (2, ROWS, 128)]
    return [pltpu.VMEM(shape, jnp.float32) for shape in shapes]


EARLY = 4


def shards(e_field, h_field, e_coef, basis, pml_width, snap_index):
    rows_count, cols_count = lax.axis_size(ROW), lax.axis_size(COL)
    full_x, full_y = 8 * rows_count, 128 * cols_count
    count = snap_index.shape[0]
    vmem = pl.BlockSpec(memory_space=pltpu.VMEM)
    smem = pl.BlockSpec(memory_space=pltpu.SMEM)
    hbm = pl.BlockSpec(memory_space=pltpu.HBM)

    turned, up, down, c_up, c_down = call(
        prepare, 10**9, PREPARE_MIB,
        out_shape=(f32(7, 8, ROWS, 128),) + (f32(7, 4, 8, 128),) * 2 + (f32(4, HALF, 128),) * 2,
        in_specs=[vmem] * 3,
        out_specs=(vmem,) * 5,
    )(e_field.reshape(3, 512, 128), h_field.reshape(3, 512, 128), e_coef.reshape(1, 512, 128))
    below, above = around(up, COL, 1), around(down, COL, -1)
    c_left, c_right = around(c_up, ROW, 1), around(c_down, ROW, -1)

    def run_alone(begin, end, turned, below, above):
        sent = f32(2 * (end - begin) * SENT + (8 * DEEP if begin == 0 else 0), 128)
        return call(
            functools.partial(alone, full_x, full_y, cols_count - 1, begin, end), 4 * 10**9, ALONE_MIB,
            out_shape=((f32(7, 8, ROWS, 128),) if begin > 0 else ()) + (sent, sent),
            in_specs=[smem] + [vmem] * 3,
            out_specs=(vmem,) * (3 if begin > 0 else 2),
            scratch_shapes=scratch(10, 1),
        )(pml_width, turned, below, above)

    up, down = run_alone(0, EARLY, turned, below, above)
    up, down, *own = lax.optimization_barrier((up, down, turned, below, above))
    left, right = around(up, ROW, 1), around(down, ROW, -1)
    turned_far, up, down = run_alone(EARLY, STEPS, *own)
    modes, up = lax.optimization_barrier((basis, up))
    modes = modes.reshape(16, rows_count, 8, 128).transpose(1, 0, 2, 3)
    modes = lax.all_to_all(modes, ROW, split_axis=0, concat_axis=0, tiled=True).reshape(1024, 128)
    up, down, left, right = lax.optimization_barrier((up, down, left, right))
    left_late, right_late = around(up, ROW, 1), around(down, ROW, -1)

    ends = call(
        functools.partial(joined, full_x, full_y, rows_count - 1, cols_count - 1, EARLY), 12 * 10**9, JOINED_MIB,
        out_shape=f32(68, ROWS, 128),
        in_specs=[smem] + [vmem] * 7,
        out_specs=vmem,
        scratch_shapes=scratch(20, 0),
    )(pml_width, turned_far, below, above, left, right, c_left, c_right)

    sums, e_final, h_final = call(
        functools.partial(late, full_x, full_y, rows_count - 1, EARLY, count), 4 * 10**9, LATE_MIB,
        out_shape=(f32(8, 12, 128), f32(1536, 128), f32(1536, 128)),
        in_specs=[smem] * 2 + [vmem] * 4,
        out_specs=(vmem, hbm, hbm),
        scratch_shapes=scratch(20, 0)
        + [
            pltpu.VMEM((6 * NZ * 8, 128), jnp.float32),
            pltpu.VMEM((count * 8, 128), jnp.float32),
            pltpu.VMEM((32, 128), jnp.float32),
            pltpu.SemaphoreType.DMA((2,)),
        ],
    )(pml_width, snap_index, ends, left_late, right_late, modes)

    part = lax.all_to_all(sums, NEAR, split_axis=0, concat_axis=0, tiled=True).sum(0)
    part = spread(part, FAR, lax.axis_size(FAR)).sum(0)
    whole = spread(part, NEAR, lax.axis_size(NEAR))
    coefficients, gram = call(
        part_out, 10**6, 4,
        out_shape=(f32(count, 128), f32(count, count)),
        in_specs=[vmem],
        out_specs=(vmem,) * 2,
    )(whole)
    shape = e_field.shape
    return (e_final.reshape(shape), h_final.reshape(shape), coefficients, gram)


PREPARE_MIB, ALONE_MIB, JOINED_MIB, LATE_MIB = 12, 14, 24, 28


def solution(mesh):
    split = Mesh(mesh.devices.reshape(4, 2, 8, 2, 2), ROW + COL)

    return jax.shard_map(
        shards,
        mesh=split,
        in_specs=(
            P(None, None, ROW, COL),
            P(None, None, ROW, COL),
            P(None, ROW, COL),
            P(ROW, None, COL),
            P(),
            P(),
        ),
        out_specs=(P(None, None, ROW, COL), P(None, None, ROW, COL), P(), P()),
        check_vma=False,
    )
```
